32 devices in a mesh: dp: 16 (over z, x, core), tensor: 2 (over y).
Axes of the slice: x: 2, y: 2, z: 4, core: 2. Of those that a mesh axis runs over, the one named last changes fastest.
Arguments:
- inputs: bfloat16 [64, 320, 1024], P(('dp', 'tensor')), may hold values from -6 to 6
- lengths: int32 [64], P('dp'), may hold values from 224 to 320, as said below
- cotangent: bfloat16 [64, 320, 1024], P(('dp', 'tensor')), may hold values from -6 to 6
- first_gain: bfloat16 [1024], P(('dp', 'tensor')), may hold values from 0.25 to 1.75
- first_shift: bfloat16 [1024], P(('dp', 'tensor')), may hold values from -2 to 2
- qkv_weight: bfloat16 [3, 1024, 1024], P(None, 'dp', 'tensor'), may hold values from -0.1875 to 0.1875
- query_bias: bfloat16 [1024], P(('dp', 'tensor')), may hold values from -3 to 3
- value_bias: bfloat16 [1024], P(('dp', 'tensor')), may hold values from -3 to 3
- out_weight: bfloat16 [1024, 1024], P('tensor', 'dp'), may hold values from -1.5 to 1.5
- out_bias: bfloat16 [1024], P(('dp', 'tensor')), may hold values from -3 to 3
- second_gain: bfloat16 [1024], P(('dp', 'tensor')), may hold values from 0.25 to 1.75
- second_shift: bfloat16 [1024], P(('dp', 'tensor')), may hold values from -2 to 2
- up_weight: bfloat16 [1024, 4096], P('dp', 'tensor'), may hold values from -0.1875 to 0.1875
- up_bias: bfloat16 [4096], P(('dp', 'tensor')), may hold values from -3 to 3
- down_weight: bfloat16 [4096, 1024], P('tensor', 'dp'), may hold values from -0.09375 to 0.09375
- down_bias: bfloat16 [1024], P(('dp', 'tensor')), may hold values from -3 to 3
Outputs:
- output: bfloat16 [64, 320, 1024], P(('dp', 'tensor'))
- input_grad: float32 [64, 320, 1024], P(('dp', 'tensor'))
- first_gain_grad: float32 [1024], P(('dp', 'tensor'))
- first_shift_grad: float32 [1024], P(('dp', 'tensor'))
- qkv_weight_grad: float32 [3, 1024, 1024], P(None, 'dp', 'tensor')
- query_bias_grad: float32 [1024], P(('dp', 'tensor'))
- value_bias_grad: float32 [1024], P(('dp', 'tensor'))
- out_weight_grad: float32 [1024, 1024], P('tensor', 'dp')
- out_bias_grad: float32 [1024], P(('dp', 'tensor'))
- second_gain_grad: float32 [1024], P(('dp', 'tensor'))
- second_shift_grad: float32 [1024], P(('dp', 'tensor'))
- up_weight_grad: float32 [1024, 4096], P('dp', 'tensor')
- up_bias_grad: float32 [4096], P(('dp', 'tensor'))
- down_weight_grad: float32 [4096, 1024], P('tensor', 'dp')
- down_bias_grad: float32 [1024], P(('dp', 'tensor'))
The draws below stay inside these ranges and needn't reach their ends.
Inputs may be any that keep to these rules, and one draw needn't show every extreme that they name: lengths holds the number of valid slots of each image, counted from its first slot; slots from there on are padding.
All inputs are finite; a program needn't handle non-finite values.
Results may differ from the reference program's by a relative error of at most 0.017.
Values may be sent and summed in bfloat16 or wider, within the bound.
A program may use at most 192 MiB of HBM per device.

```python
import jax
import jax.numpy as jnp
from jax import lax

D = 1024
HEADS = 16
HEAD_DIM = 64
FF = 4096
SLOTS = 320
MIN_LEN = 224
IMAGES = 64


def draw_lengths(key, part):
    drawn = jax.random.randint(key, (IMAGES,), MIN_LEN, SLOTS + 1, dtype=jnp.int32)
    drawn = drawn.at[0].set(SLOTS)
    drawn = drawn.at[1].set(MIN_LEN)
    return drawn


def spiked(values, key, source, target, shards_of, factor):
    def block_of(dim):
        return (jnp.arange(values.shape[dim]) // (values.shape[dim] // shards_of)).reshape((-1,) + (1,) * (values.ndim - 1 - dim))

    one_side = jax.random.permutation(key, shards_of)[block_of(target)]
    far = (block_of(target) + shards_of // 2) % shards_of
    return jnp.where((block_of(source) == one_side) | (block_of(source) == far), factor * values, values)


def block_levels(stream_key, dims, cuts, smallest, high):
    def one(dim, parts):
        steps = jax.random.uniform(jax.random.fold_in(jax.random.fold_in(stream_key, 6), dim), (parts,), jnp.float32, smallest / len(cuts), high / len(cuts))
        return jnp.repeat(jnp.exp(steps), dims[dim] // parts).reshape((-1,) + (1,) * (len(dims) - dim - 1))

    loudness = one(*cuts[0])
    for cut in cuts[1:]:
        loudness = loudness * one(*cut)
    return loudness


def centred(stream_key, shape, width, most, shards=(), kind=jnp.bfloat16):
    level = block_levels(stream_key, shape, shards, -0.22, 0.18) if shards else 1.0
    entries = jax.random.normal(stream_key, shape, jnp.float32) * width * level
    return jnp.minimum(jnp.maximum(entries, -most), most).astype(kind)


def bell_draw_with(key, dims, width, limit, cuts, heavy, kind=jnp.bfloat16):
    entries = width * jax.random.normal(key, dims, jnp.float32)
    if cuts:
        entries = entries * block_levels(key, dims, cuts, -0.22, 0.18)
    return jnp.clip(spiked(entries, jax.random.fold_in(key, 3), *heavy), -limit, limit).astype(kind)


def setup_inputs(seed: int = 0) -> dict:
    key_list = jax.random.split(jax.random.key(seed), 17)
    inputs = centred(key_list[0], (IMAGES, SLOTS, D), 1.0, 6.0, ((0, 32),))
    lengths = draw_lengths(jax.random.fold_in(key_list[16], 71), 0)
    cotangent = bell_draw_with(key_list[2], (IMAGES, SLOTS, D), 1.0, 6.0, ((0, 32),), (0, 2, 32, 2.75))
    first_gain = jnp.clip(1.0 + 0.15 * jax.random.normal(key_list[3], (D,), jnp.float32), 0.25, 1.75).astype(jnp.bfloat16)
    first_shift = centred(key_list[4], (D,), 0.3, 2.0, ((0, 32),))
    qkv_weight = centred(key_list[5], (3, D, D), D ** -0.5, 0.1875, ((1, 16), (2, 2)))
    query_bias = centred(key_list[6], (D,), 0.5, 3.0, ((0, 32),))
    value_bias = centred(key_list[7], (D,), 0.5, 3.0, ((0, 32),))
    out_weight = centred(key_list[8], (D, D), (D // 64) ** -0.5, 1.5, ((0, 2), (1, 16)))
    out_bias = centred(key_list[9], (D,), 0.5, 3.0, ((0, 32),))
    second_gain = jnp.clip(1.0 + 0.15 * jax.random.normal(key_list[10], (D,), jnp.float32), 0.25, 1.75).astype(jnp.bfloat16)
    second_shift = centred(key_list[11], (D,), 0.3, 2.0, ((0, 32),))
    up_weight = centred(key_list[12], (D, FF), D ** -0.5, 0.1875, ((0, 16), (1, 2)))
    up_bias = centred(key_list[13], (FF,), 0.5, 3.0, ((0, 32),))
    down_weight = centred(key_list[14], (FF, D), FF ** -0.5, 0.09375, ((0, 2), (1, 16)))
    down_bias = centred(key_list[15], (D,), 0.5, 3.0, ((0, 32),))
    return dict(inputs=inputs, lengths=lengths, cotangent=cotangent, first_gain=first_gain, first_shift=first_shift, qkv_weight=qkv_weight, query_bias=query_bias, value_bias=value_bias, out_weight=out_weight, out_bias=out_bias, second_gain=second_gain, second_shift=second_shift, up_weight=up_weight, up_bias=up_bias, down_weight=down_weight, down_bias=down_bias)


@jax.custom_vjp
def low(v):
    return lax.optimization_barrier(v.astype(jnp.bfloat16)).astype(jnp.float32)

@jax.custom_vjp
def low_back(v):
    return v

def low_keep(v):
    return (low(v), None)

def low_pass(kept, grad):
    return (grad,)

def back_keep(v):
    return (v, None)

def back_low(kept, grad):
    return (low(grad),)
low.defvjp(low_keep, low_pass)
low_back.defvjp(back_keep, back_low)
EPSILON = 1e-06
HIGHEST = lax.Precision.HIGHEST

def norm_rows(values, gain, shift):
    average = lax.optimization_barrier(jnp.mean(values, axis=-1, keepdims=True))
    centered = values - average
    variance = lax.optimization_barrier(jnp.mean(centered * centered, axis=-1, keepdims=True))
    return centered * lax.rsqrt(variance + EPSILON) * gain + shift

def project(rows, matrix):
    return jnp.einsum('bsd,de->bse', rows, matrix, precision=HIGHEST)

def layer(masked, key_valid, first_gain, first_shift, qkv_weight, query_bias, value_bias, out_weight, out_bias, second_gain, second_shift, up_weight, up_bias, down_weight, down_bias):
    group_count, slot_count, model_width = masked.shape
    first_normed = low(norm_rows(masked, first_gain, first_shift))
    query_rows = low_back(low(project(first_normed, qkv_weight[0]) + query_bias))
    key_rows = low_back(low(project(first_normed, qkv_weight[1])))
    value_rows = low_back(low(project(first_normed, qkv_weight[2]) + value_bias))
    query_heads = query_rows.reshape(group_count, slot_count, HEADS, HEAD_DIM)
    key_heads = key_rows.reshape(group_count, slot_count, HEADS, HEAD_DIM)
    value_heads = value_rows.reshape(group_count, slot_count, HEADS, HEAD_DIM)
    scores = low_back(HEAD_DIM ** (-0.5) * jnp.einsum('bqhc,bkhc->bhqk', query_heads, key_heads, precision=HIGHEST))
    scores = jnp.where(key_valid[:, None, None, :], scores, -1000000000.0)
    weights_low = low(jax.nn.softmax(scores, axis=-1))
    mixed = jnp.einsum('bhqk,bkhc->bqhc', weights_low, value_heads, precision=HIGHEST)
    mixed = low_back(low(mixed.reshape(group_count, slot_count, model_width)))
    middle = masked + low_back(project(mixed, out_weight) + out_bias)
    second_normed = low(norm_rows(middle, second_gain, second_shift))
    hidden = low_back(project(second_normed, up_weight) + up_bias)
    active = low(jax.nn.gelu(hidden, approximate=False))
    return middle + low_back(project(active, down_weight) + down_bias)

def reference(inputs, lengths, cotangent, first_gain, first_shift, qkv_weight, query_bias, value_bias, out_weight, out_bias, second_gain, second_shift, up_weight, up_bias, down_weight, down_bias):
    positions = jnp.arange(SLOTS, dtype=jnp.int32)
    valid = positions[None, :] < lengths.astype(jnp.int32)[:, None]
    valid_float = valid.astype(jnp.float32)[:, :, None]
    params = tuple((member.astype(jnp.float32) for member in (first_gain, first_shift, qkv_weight, query_bias, value_bias, out_weight, out_bias, second_gain, second_shift, up_weight, up_bias, down_weight, down_bias)))
    masked = inputs.astype(jnp.float32) * valid_float
    grad_out = cotangent.astype(jnp.float32)
    groups = IMAGES // 8

    def one_group(carry, pieces):
        block_in, block_valid, block_grad = pieces

        def apply(block, *weights):
            return layer(block, block_valid, *weights)
        block_out, pull = jax.vjp(apply, block_in, *params)
        grads = pull(block_grad)
        new_carry = tuple((total + term for total, term in zip(carry, grads[1:])))
        return (new_carry, (block_out, grads[0]))
    zeros = tuple((jnp.zeros(member.shape, jnp.float32) for member in params))
    totals, (outs, input_terms) = lax.scan(one_group, zeros, (masked.reshape(groups, 8, SLOTS, D), valid.reshape(groups, 8, SLOTS), grad_out.reshape(groups, 8, SLOTS, D)))
    output = outs.reshape(IMAGES, SLOTS, D).astype(jnp.bfloat16)
    input_grad = input_terms.reshape(IMAGES, SLOTS, D) * valid_float
    return (output, input_grad, totals[0], totals[1], totals[2], totals[3], totals[4], totals[5], totals[6], totals[7], totals[8], totals[9], totals[10], totals[11], totals[12])
```

```python
import jax
import jax.numpy as jnp
from jax import lax
from jax.sharding import PartitionSpec as P

HEAD_DIM = 64
EPSILON = 1e-06
BOTH = ("dp", "tensor")
bf16 = jnp.bfloat16
f32 = jnp.float32


def exact_gelu(values):
    return jax.nn.gelu(values, approximate=False)


def norm_stats(values):
    average = jnp.mean(values, axis=-1, keepdims=True)
    centered = values - average
    variance = jnp.mean(centered * centered, axis=-1, keepdims=True)
    scale = lax.rsqrt(variance + EPSILON)
    return centered * scale, scale


def norm_back(grad, unit, scale, gain):
    z = grad * gain
    mean_z = jnp.mean(z, axis=-1, keepdims=True)
    mean_zx = jnp.mean(z * unit, axis=-1, keepdims=True)
    return scale * (z - mean_z - unit * mean_zx)


def gather_matrix(shard):
    wide = lax.all_gather(shard, "tensor", axis=1, tiled=True)
    return lax.all_gather(wide, "dp", axis=0, tiled=True)


def scatter_matrix(grad):
    rows, columns = grad.shape
    halves = jnp.stack(jnp.split(grad, lax.axis_size("tensor"), axis=1))
    halves = halves.reshape(-1, columns // lax.axis_size("tensor"))
    return lax.psum_scatter(halves, ("tensor", "dp"), scatter_dimension=0, tiled=True)


def mm(a, b, dims):
    return lax.dot_general(a, b, (dims, ((), ())), preferred_element_type=f32)


NN = ((1,), (0,))
NT = ((1,), (1,))
TN = ((0,), (0,))


def shards(
    inputs,
    lengths,
    cotangent,
    first_gain,
    first_shift,
    qkv_weight,
    query_bias,
    value_bias,
    out_weight,
    out_bias,
    second_gain,
    second_shift,
    up_weight,
    up_bias,
    down_weight,
    down_bias,
):
    image_count, slot_count, width = inputs.shape
    tensor_rank = lax.axis_index("tensor")
    heads = width // HEAD_DIM
    tokens = image_count * slot_count
    score_scale = HEAD_DIM ** (-0.5)
    device_count = lax.axis_size("dp") * lax.axis_size("tensor")

    vectors = (
        first_gain,
        first_shift,
        query_bias,
        value_bias,
        out_bias,
        second_gain,
        second_shift,
        down_bias,
        up_bias,
    )
    sizes = [v.shape[0] for v in vectors]
    packed = lax.all_gather(jnp.concatenate(vectors), BOTH, axis=0)
    full = []
    start = 0
    for size in sizes:
        full.append(packed[:, start : start + size].reshape(-1).astype(f32))
        start += size
    gain_one, shift_one, qbias, vbias, obias, gain_two, shift_two, dbias, ubias = full

    query_w = gather_matrix(qkv_weight[0])
    key_w = gather_matrix(qkv_weight[1])
    value_w = gather_matrix(qkv_weight[2])
    out_t = gather_matrix(out_weight.T)
    up_w = gather_matrix(up_weight)
    down_t = gather_matrix(down_weight.T)

    positions = jnp.arange(slot_count, dtype=jnp.int32)
    own_lengths = lax.dynamic_slice_in_dim(lengths, tensor_rank * image_count, image_count)
    valid = positions[None, :] < own_lengths[:, None]
    valid_rows = valid.astype(f32).reshape(tokens, 1)
    masked = inputs.reshape(tokens, width).astype(f32) * valid_rows
    unit_one, scale_one = norm_stats(masked)
    first = (unit_one * gain_one + shift_one).astype(bf16)

    def split(rows):
        return rows.reshape(image_count, slot_count, heads, HEAD_DIM)

    query = split((mm(first, query_w, NN) + qbias).astype(bf16))
    key = split(mm(first, key_w, NN).astype(bf16))
    value = split((mm(first, value_w, NN) + vbias).astype(bf16))
    scores = jnp.einsum("bqhc,bkhc->bhqk", query, key, preferred_element_type=f32) * score_scale
    scores = jnp.where(valid[:, None, None, :], scores, -1000000000.0)
    highest = jnp.max(scores, axis=-1, keepdims=True)
    shifted = jnp.exp(scores - highest)
    probs = shifted / jnp.sum(shifted, axis=-1, keepdims=True)
    weights_low = probs.astype(bf16)
    mixed = jnp.einsum("bhqk,bkhc->bqhc", weights_low, value, preferred_element_type=f32)
    mixed = mixed.astype(bf16).reshape(tokens, width)
    middle = masked + mm(mixed, out_t, NT) + obias
    unit_two, scale_two = norm_stats(middle)
    second = (unit_two * gain_two + shift_two).astype(bf16)
    hidden = mm(second, up_w, NN) + ubias
    active = exact_gelu(hidden).astype(bf16)
    output = (middle + mm(active, down_t, NT) + dbias).astype(bf16)

    grad_low = cotangent.reshape(tokens, width)
    grad_out = grad_low.astype(f32)
    down_grad = scatter_matrix(mm(grad_low, active, TN).astype(bf16))
    grad_active = mm(grad_low, down_t, NN)
    grad_hidden32 = jax.vjp(exact_gelu, hidden)[1](grad_active)[0]
    grad_hidden = grad_hidden32.astype(bf16)
    up_grad = scatter_matrix(mm(second, grad_hidden, TN).astype(bf16))
    grad_second = mm(grad_hidden, up_w, NT)
    grad_middle = grad_out + norm_back(grad_second, unit_two, scale_two, gain_two)
    grad_attn = grad_middle.astype(bf16)
    out_grad = scatter_matrix(mm(grad_attn, mixed, TN).astype(bf16))
    grad_mixed = split(mm(grad_attn, out_t, NN).astype(bf16))
    grad_weights = jnp.einsum("bqhc,bkhc->bhqk", grad_mixed, value, preferred_element_type=f32)
    value_grad = jnp.einsum("bhqk,bqhc->bkhc", weights_low, grad_mixed, preferred_element_type=f32)
    value_grad = value_grad.astype(bf16).reshape(tokens, width)
    inner = jnp.sum(probs * grad_weights, axis=-1, keepdims=True)
    grad_scores = (probs * (grad_weights - inner)).astype(bf16)
    query_grad = (
        jnp.einsum("bhqk,bkhc->bqhc", grad_scores, key, preferred_element_type=f32) * score_scale
    )
    key_grad = (
        jnp.einsum("bhqk,bqhc->bkhc", grad_scores, query, preferred_element_type=f32) * score_scale
    )
    query_grad = query_grad.astype(bf16).reshape(tokens, width)
    key_grad = key_grad.astype(bf16).reshape(tokens, width)
    qkv_grad = jnp.stack(
        [
            scatter_matrix(mm(first, query_grad, TN).astype(bf16)),
            scatter_matrix(mm(first, key_grad, TN).astype(bf16)),
            scatter_matrix(mm(first, value_grad, TN).astype(bf16)),
        ]
    )
    grad_first = mm(query_grad, query_w, NT) + mm(key_grad, key_w, NT) + mm(value_grad, value_w, NT)
    grad_in = norm_back(grad_first, unit_one, scale_one, gain_one)
    input_grad = (grad_middle + grad_in) * valid_rows

    def total(values):
        return jnp.sum(values.astype(f32), axis=0)

    vector_grads = (
        total(grad_first * unit_one),
        total(grad_first),
        total(query_grad),
        total(value_grad),
        total(grad_attn),
        total(grad_second * unit_two),
        total(grad_second),
        total(grad_low),
        total(grad_hidden),
    )
    stacked = jnp.concatenate([v.reshape(device_count, -1) for v in vector_grads], axis=1)
    own = lax.psum_scatter(stacked, BOTH, scatter_dimension=0, tiled=True)[0]
    shares = []
    start = 0
    for size in sizes:
        shares.append(own[start : start + size])
        start += size

    return (
        output.reshape(inputs.shape),
        input_grad.reshape(inputs.shape),
        shares[0],
        shares[1],
        qkv_grad.astype(f32),
        shares[2],
        shares[3],
        out_grad.T.astype(f32),
        shares[4],
        shares[5],
        shares[6],
        up_grad.astype(f32),
        shares[8],
        down_grad.T.astype(f32),
        shares[7],
    )


def solution(mesh):
    rows = P(BOTH, None, None)
    vector = P(BOTH)
    return jax.shard_map(
        shards,
        mesh=mesh,
        in_specs=(
            rows,
            P("dp"),
            rows,
            vector,
            vector,
            P(None, "dp", "tensor"),
            vector,
            vector,
            P("tensor", "dp"),
            vector,
            vector,
            vector,
            P("dp", "tensor"),
            vector,
            P("tensor", "dp"),
            vector,
        ),
        out_specs=(
            rows,
            rows,
            vector,
            vector,
            P(None, "dp", "tensor"),
            vector,
            vector,
            P("tensor", "dp"),
            vector,
            vector,
            vector,
            P("dp", "tensor"),
            vector,
            P("tensor", "dp"),
            vector,
        ),
        check_vma=False,
    )
```

```python
import functools
import math

import jax
import jax.numpy as jnp
from jax import lax
from jax.experimental import pallas as pl
from jax.experimental.pallas import tpu as pltpu
from jax.sharding import PartitionSpec as P

HEAD_DIM = 64
EPSILON = 1e-06
BOTH = ("dp", "tensor")
MESH = pl.DeviceIdType.MESH
LANES = 128
bf16 = jnp.bfloat16
f32 = jnp.float32


class Place:
    def __init__(self, dp_count):
        self.bits = int(math.log2(dp_count))
        self.dp = lax.axis_index("dp")
        self.tensor = lax.axis_index("tensor")
        self.own = [lax.rem(lax.div(self.dp, 2**k), 2) for k in range(self.bits)]

    def partner(self, stage):
        if stage == "t":
            return {"tensor": 1 - self.tensor}
        return {"dp": self.dp + (1 - 2 * self.own[stage]) * 2**stage}

    def greet(self):
        barrier = pltpu.get_barrier_semaphore()
        stages = list(range(self.bits)) + ["t"]
        for stage in stages:
            pl.semaphore_signal(barrier, inc=1, device_id=self.partner(stage), device_id_type=MESH)
        pl.semaphore_wait(barrier, len(stages))

    def lead(self, done, flipped=None):
        index = []
        for bit in range(self.bits - 1, -1, -1):
            if bit in done:
                index.append(slice(None))
            elif bit == flipped:
                index.append(1 - self.own[bit])
            else:
                index.append(self.own[bit])
        return tuple(index)


def stage_orders(bits):
    far = list(range(bits - 1, 1, -1))
    return (far + [1, "t"], far + ["t", 1], [1] + far + ["t"], ["t"] + far + [1])


class Spread:
    def __init__(self, place, shard, full, half, first, count, order, sems, base):
        self.place, self.shard, self.full = place, shard, full
        self.half, self.first, self.count, self.order = half, first, count, order
        self.send, self.recv, self.local = sems
        self.slot = base
        self.stages = len(order)
        self.plane = [None] * self.stages
        self.across = []

    @staticmethod
    def slots(order):
        total, twice = 1, 1
        for stage in order:
            total += twice
            total += twice
            if stage == "t":
                twice = 2
        return total

    def columns(self, which):
        return pl.ds(pl.multiple_of(which * self.half + self.first, 128), self.count)

    def views(self, done, flipped=None):
        place = self.place
        if "t" in done:
            sides = [0, 1]
        elif flipped == "t":
            sides = [1 - place.tensor]
        else:
            sides = [place.tensor]
        lead = place.lead(done, flipped)
        return [self.full.at[lead + (slice(None), self.columns(side))] for side in sides]

    def post(self, src, dst, stage):
        made = pltpu.make_async_remote_copy(
            src_ref=src,
            dst_ref=dst,
            send_sem=self.send.at[self.slot],
            recv_sem=self.recv.at[self.slot],
            device_id=self.place.partner(stage),
            device_id_type=MESH,
        )
        self.slot += 1
        made.start()
        return made

    def piece(self):
        return self.shard.at[:, pl.ds(self.first, self.count)]

    def tick(self, step):
        order = self.order
        if step == 0:
            (target,) = self.views(set())
            self.keep = pltpu.make_async_copy(self.piece(), target, self.local)
            self.keep.start()
            self.plane[0] = [self.post(self.piece(), target, order[0])]
            self.across.append(self.post(self.piece(), target, 0))
            return
        for made in self.plane[step - 1]:
            made.wait_recv()
        if step == 1:
            self.keep.wait()
        before = set(order[: step - 1])
        if step < self.stages:
            held = self.views(before | {order[step - 1]})
            self.plane[step] = [self.post(view, view, order[step]) for view in held]
        fresh = self.views(before, order[step - 1])
        self.across.extend(self.post(view, view, 0) for view in fresh)

    def finish(self):
        for group in self.plane:
            for made in group:
                made.wait_send()
        for made in self.across:
            made.wait()


def spread_kernel(plan, dp_count, names, *refs):
    count = names
    shards, fulls = refs[:count], refs[count : 2 * count]
    send, recv, local = refs[2 * count :]
    place = Place(dp_count)
    place.greet()
    orders = stage_orders(place.bits)
    flows, base = [], 0
    for index, (matrix, first, columns, which, begin) in enumerate(plan):
        order = orders[which]
        shard = shards[matrix]
        sems = (send, recv, local.at[index])
        flows.append(
            (begin, Spread(place, shard, fulls[matrix], shard.shape[1], first, columns, order, sems, base))
        )
        base += Spread.slots(order)
    last = max(begin for begin, _ in flows) + len(orders[0])
    for tick in range(last + 1):
        for begin, flow in flows:
            if 0 <= tick - begin <= flow.stages:
                flow.tick(tick - begin)
    for _, flow in flows:
        flow.finish()


def spread_matrices(shards, plan, collective_id):
    dp_count = lax.axis_size("dp")
    bits = int(math.log2(dp_count))
    orders = stage_orders(bits)
    slots = sum(Spread.slots(orders[entry[3]]) for entry in plan)
    sent = 0
    fulls = pl.pallas_call(
        functools.partial(spread_kernel, plan, dp_count, len(shards)),
        out_shape=[
            jax.ShapeDtypeStruct((2,) * bits + (s.shape[0], 2 * s.shape[1]), s.dtype) for s in shards
        ],
        in_specs=[pl.BlockSpec(memory_space=pltpu.VMEM)] * len(shards),
        out_specs=[pl.BlockSpec(memory_space=pl.ANY)] * len(shards),
        scratch_shapes=[
            pltpu.SemaphoreType.DMA((slots,)),
            pltpu.SemaphoreType.DMA((slots,)),
            pltpu.SemaphoreType.DMA((len(plan),)),
        ],
        compiler_params=pltpu.CompilerParams(collective_id=collective_id, has_side_effects=True, vmem_limit_bytes=8 << 20),
        name="spread_weights",
    )(*shards)
    return [f.reshape(dp_count * s.shape[0], 2 * s.shape[1]) for f, s in zip(fulls, shards)]


class Fold:
    def __init__(self, place, partial, half, first, count, order, refs, sems, base):
        self.place, self.partial = place, partial
        self.half, self.first, self.count = half, first, count
        self.order = list(reversed(order))
        self.total, self.landing, self.result = refs
        self.send, self.recv, self.local = sems
        self.slot = base
        self.stages = len(order)
        self.copies = []

    @staticmethod
    def slots(order):
        return 2 + len(order)

    def post(self, src, dst, stage):
        made = pltpu.make_async_remote_copy(
            src_ref=src,
            dst_ref=dst,
            send_sem=self.send.at[self.slot],
            recv_sem=self.recv.at[self.slot],
            device_id=self.place.partner(stage),
            device_id_type=MESH,
        )
        self.slot += 1
        made.start()
        return made

    def begin(self):
        place = self.place
        every = set(range(1, place.bits))
        self.loads, self.cores = [], []
        for side in (0, 1):
            columns = pl.ds(side * self.half + self.first, self.count)
            mine = self.partial.at[place.lead(every) + (slice(None), columns)]
            theirs = self.partial.at[place.lead(every, 0) + (slice(None), columns)]
            self.cores.append(self.post(theirs, self.landing[0].at[side], 0))
            load = pltpu.make_async_copy(mine, self.total.at[side], self.local.at[side])
            load.start()
            self.loads.append(load)

    def where(self, done, last=None):
        place = self.place
        index = []
        for name in ["t"] + list(range(place.bits - 1, 0, -1)):
            own = place.tensor if name == "t" else place.own[name]
            if name in done:
                index.append(own)
            elif name == last:
                index.append(1 - own)
            else:
                index.append(None)
        return index

    def add(self, landing, done):
        index = self.where(done)
        free = [i for i, entry in enumerate(index) if entry is None]
        size = 2 ** len(free)

        def one(j, carry):
            spots, inner = list(index), []
            for position, dim in enumerate(free):
                bit = lax.rem(lax.div(j, 2 ** (len(free) - 1 - position)), 2)
                spots[dim] = bit
                inner.append(bit)
            spots, inner = tuple(spots), tuple(inner)
            value = self.total[spots].astype(f32) + landing[inner].astype(f32)
            self.total[spots] = value.astype(self.total.dtype)
            return carry

        lax.fori_loop(0, size, one, 0)

    def tick(self, step):
        order = self.order
        if step == 0:
            for load in self.loads:
                load.wait()
            for made in self.cores:
                made.wait_recv()
            self.add(self.landing[0], set())
        else:
            self.copies[step - 1].wait_recv()
            if step < self.stages:
                self.add(self.landing[step], set(order[:step]))
            else:
                spots = tuple(self.where(set(order)))
                value = self.total[spots].astype(f32) + self.landing[step][...].astype(f32)
                self.result[:, self.first : self.first + self.count] = value
        if step < self.stages:
            index = self.where(set(order[:step]), order[step])
            view = self.total.at[tuple(slice(None) if e is None else e for e in index)]
            self.copies.append(self.post(view, self.landing[step + 1], order[step]))

    def finish(self):
        for made in self.cores + self.copies:
            made.wait_send()


def fold_scratch(bits, rows, count, dtype):
    lead = (2,) * bits
    shapes = [pltpu.VMEM(lead + (rows, count), dtype)]
    shapes.append(pltpu.VMEM(lead + (rows, count), dtype))
    for stage in range(1, bits + 1):
        shapes.append(pltpu.VMEM(lead[stage:] + (rows, count), dtype))
    return shapes


def fold_kernel(plan, dp_count, count, *refs):
    place = Place(dp_count)
    bits = place.bits
    partials, results = refs[:count], refs[count : 2 * count]
    send, recv, local = refs[2 * count : 2 * count + 3]
    buffers = refs[2 * count + 3 :]
    place.greet()
    orders = stage_orders(bits)
    flows, base = [], 0
    for index, (matrix, first, columns, which, begin) in enumerate(plan):
        order = orders[which]
        mine = buffers[index * (bits + 2) : (index + 1) * (bits + 2)]
        half = partials[matrix].shape[-1] // 2
        sems = (send, recv, local.at[index])
        refs_here = (mine[0], mine[1:], results[matrix])
        flow = Fold(place, partials[matrix], half, first, columns, order, refs_here, sems, base)
        flows.append((begin, flow))
        base += Fold.slots(order)
    for _, flow in flows:
        flow.begin()
    last = max(begin for begin, _ in flows) + len(orders[0])
    for tick in range(last + 1):
        for begin, flow in flows:
            if 0 <= tick - begin <= flow.stages:
                flow.tick(tick - begin)
    for _, flow in flows:
        flow.finish()


def fold_matrices(partials, plan, collective_id):
    dp_count = lax.axis_size("dp")
    bits = int(math.log2(dp_count))
    orders = stage_orders(bits)
    slots = sum(Fold.slots(orders[entry[3]]) for entry in plan)
    views = []
    for p in partials:
        rows = p.shape[0] // dp_count
        views.append(p.reshape((2,) * bits + (rows, p.shape[1])))
    scratch = [
        pltpu.SemaphoreType.DMA((slots,)),
        pltpu.SemaphoreType.DMA((slots,)),
        pltpu.SemaphoreType.DMA((len(plan), 2)),
    ]
    for matrix, first, columns, which, begin in plan:
        scratch += fold_scratch(bits, views[matrix].shape[-2], columns, views[matrix].dtype)
    return pl.pallas_call(
        functools.partial(fold_kernel, plan, dp_count, len(views)),
        out_shape=[jax.ShapeDtypeStruct((v.shape[-2], v.shape[-1] // 2), f32) for v in views],
        in_specs=[pl.BlockSpec(memory_space=pl.ANY)] * len(views),
        out_specs=[pl.BlockSpec(memory_space=pltpu.VMEM)] * len(views),
        scratch_shapes=scratch,
        compiler_params=pltpu.CompilerParams(
            collective_id=collective_id, has_side_effects=True, vmem_limit_bytes=56 << 20
        ),
        name="fold_grads",
    )(*views)


def make_plan(sizes, fractions):
    plan, position, tick = [], {}, 0
    for matrix, size in sizes:
        start = position.get(matrix, 0)
        units, total, taken, gone = size // 128, sum(fractions), 0, 0
        for which, weight in enumerate(fractions):
            taken += weight
            upto = (units * taken * 2 + total) // (2 * total)
            if upto > gone:
                plan.append((matrix, start + gone * 128, (upto - gone) * 128, which, tick))
            gone = upto
        position[matrix] = start + size
        tick += 1
    return plan


EVEN = (1, 1, 1, 1)


def chunks(order, halves):
    sizes = []
    for matrix in order:
        half = halves[matrix]
        if half > 1536:
            sizes += [(matrix, half // 2)] * 2
        else:
            sizes.append((matrix, half))
    return sizes


def exact_gelu(values):
    return jax.nn.gelu(values, approximate=False)


def norm_stats(values):
    average = jnp.mean(values, axis=-1, keepdims=True)
    centered = values - average
    variance = jnp.mean(centered * centered, axis=-1, keepdims=True)
    scale = lax.rsqrt(variance + EPSILON)
    return centered * scale, scale


def norm_back(grad, unit, scale, gain):
    z = grad * gain
    mean_z = jnp.mean(z, axis=-1, keepdims=True)
    mean_zx = jnp.mean(z * unit, axis=-1, keepdims=True)
    return scale * (z - mean_z - unit * mean_zx)


def mm(a, b, dims):
    return lax.dot_general(a, b, (dims, ((), ())), preferred_element_type=f32)


NN = ((1,), (0,))
NT = ((1,), (1,))
TN = ((0,), (0,))


def shards(
    inputs,
    lengths,
    cotangent,
    first_gain,
    first_shift,
    qkv_weight,
    query_bias,
    value_bias,
    out_weight,
    out_bias,
    second_gain,
    second_shift,
    up_weight,
    up_bias,
    down_weight,
    down_bias,
):
    image_count, slot_count, width = inputs.shape
    tensor_rank = lax.axis_index("tensor")
    heads = width // HEAD_DIM
    tokens = image_count * slot_count
    score_scale = HEAD_DIM ** (-0.5)
    device_count = lax.axis_size("dp") * lax.axis_size("tensor")

    vectors = (
        first_gain,
        first_shift,
        query_bias,
        value_bias,
        out_bias,
        second_gain,
        second_shift,
        down_bias,
        up_bias,
    )
    sizes = [v.shape[0] for v in vectors]
    packed = jnp.concatenate(vectors)
    length = -(-packed.shape[0] // LANES) * LANES
    packed = jnp.pad(packed, (0, length - packed.shape[0]))
    part = width // lax.axis_size("tensor")
    row_count = qkv_weight.shape[1]
    shards_here = [
        qkv_weight.transpose(1, 0, 2).reshape(row_count, 3 * part),
        out_weight.T,
        up_weight,
        down_weight.T,
        jnp.broadcast_to(packed, (8, length)),
    ]
    halves = [s.shape[1] for s in shards_here]
    plan = [(4, 0, length, 2, 0)] + make_plan(chunks((0, 1, 2, 3), halves), EVEN)
    qkv_w, out_t, up_w, down_t, spread = spread_matrices(shards_here, plan, 1)
    spread = spread.reshape(-1, 8, 2, length)[:, 0].reshape(device_count, length)
    full = []
    start = 0
    for size in sizes:
        full.append(spread[:, start : start + size].reshape(-1).astype(f32))
        start += size
    gain_one, shift_one, qbias, vbias, obias, gain_two, shift_two, dbias, ubias = full

    positions = jnp.arange(slot_count, dtype=jnp.int32)
    own_lengths = lax.dynamic_slice_in_dim(lengths, tensor_rank * image_count, image_count)
    valid = positions[None, :] < own_lengths[:, None]
    valid_rows = valid.astype(f32).reshape(tokens, 1)
    masked = inputs.reshape(tokens, width).astype(f32) * valid_rows
    unit_one, scale_one = norm_stats(masked)
    first = (unit_one * gain_one + shift_one).astype(bf16)

    def split(rows):
        return rows.reshape(image_count, slot_count, heads, HEAD_DIM)

    rows = mm(first, qkv_w, NN).reshape(tokens, 2, 3, part)
    query = split((rows[:, :, 0].reshape(tokens, width) + qbias).astype(bf16))
    key = split(rows[:, :, 1].reshape(tokens, width).astype(bf16))
    value = split((rows[:, :, 2].reshape(tokens, width) + vbias).astype(bf16))
    scores = jnp.einsum("bqhc,bkhc->bhqk", query, key, preferred_element_type=f32) * score_scale
    scores = jnp.where(valid[:, None, None, :], scores, -1000000000.0)
    highest = jnp.max(scores, axis=-1, keepdims=True)
    shifted = jnp.exp(scores - highest)
    probs = shifted / jnp.sum(shifted, axis=-1, keepdims=True)
    weights_low = probs.astype(bf16)
    mixed = jnp.einsum("bhqk,bkhc->bqhc", weights_low, value, preferred_element_type=f32)
    mixed = mixed.astype(bf16).reshape(tokens, width)
    middle = masked + mm(mixed, out_t, NT) + obias
    unit_two, scale_two = norm_stats(middle)
    second = (unit_two * gain_two + shift_two).astype(bf16)
    hidden = mm(second, up_w, NN) + ubias
    active = exact_gelu(hidden).astype(bf16)
    output = (middle + mm(active, down_t, NT) + dbias).astype(bf16)

    grad_low = cotangent.reshape(tokens, width)
    grad_out = grad_low.astype(f32)
    down_part = mm(grad_low, active, TN).astype(bf16)
    grad_active = mm(grad_low, down_t, NN)
    grad_hidden32 = jax.vjp(exact_gelu, hidden)[1](grad_active)[0]
    grad_hidden = grad_hidden32.astype(bf16)
    up_part = mm(second, grad_hidden, TN).astype(bf16)
    grad_second = mm(grad_hidden, up_w, NT)
    grad_middle = grad_out + norm_back(grad_second, unit_two, scale_two, gain_two)
    grad_attn = grad_middle.astype(bf16)
    out_part = mm(grad_attn, mixed, TN).astype(bf16)
    grad_mixed = split(mm(grad_attn, out_t, NN).astype(bf16))
    grad_weights = jnp.einsum("bqhc,bkhc->bhqk", grad_mixed, value, preferred_element_type=f32)
    value_grad = jnp.einsum("bhqk,bqhc->bkhc", weights_low, grad_mixed, preferred_element_type=f32)
    value_grad = value_grad.astype(bf16).reshape(tokens, width)
    inner = jnp.sum(probs * grad_weights, axis=-1, keepdims=True)
    grad_scores = (probs * (grad_weights - inner)).astype(bf16)
    query_grad = (
        jnp.einsum("bhqk,bkhc->bqhc", grad_scores, key, preferred_element_type=f32) * score_scale
    )
    key_grad = (
        jnp.einsum("bhqk,bqhc->bkhc", grad_scores, query, preferred_element_type=f32) * score_scale
    )
    query_grad = query_grad.astype(bf16).reshape(tokens, width)
    key_grad = key_grad.astype(bf16).reshape(tokens, width)
    grad_rows = jnp.stack(
        [g.reshape(tokens, 2, part) for g in (query_grad, key_grad, value_grad)], axis=2
    ).reshape(tokens, 3 * width)
    qkv_part = mm(first, grad_rows, TN).astype(bf16)
    grad_first = mm(grad_rows, qkv_w, NT)
    grad_in = norm_back(grad_first, unit_one, scale_one, gain_one)
    input_grad = (grad_middle + grad_in) * valid_rows

    def total(values):
        return jnp.sum(values.astype(f32), axis=0)

    vector_grads = (
        total(grad_first * unit_one),
        total(grad_first),
        total(query_grad),
        total(value_grad),
        total(grad_attn),
        total(grad_second * unit_two),
        total(grad_second),
        total(grad_low),
        total(grad_hidden),
    )
    stacked = jnp.concatenate([v.reshape(device_count, -1) for v in vector_grads], axis=1)
    stacked = jnp.pad(stacked, ((0, 0), (0, length - stacked.shape[1])))
    stacked = stacked.reshape(-1, 1, 2 * length)
    stacked = jnp.pad(stacked, ((0, 0), (0, 7), (0, 0))).reshape(-1, 2 * length)
    plan = make_plan(chunks((3, 2, 1, 0), halves), EVEN)
    plan = plan + [(4, 0, length, 2, 0)]
    qkv_grad, out_grad, up_grad, down_grad, own = fold_matrices(
        [qkv_part, out_part, up_part, down_part, stacked], plan, 2
    )
    own = own[0]
    shares = []
    start = 0
    for size in sizes:
        shares.append(own[start : start + size])
        start += size

    return (
        output.reshape(inputs.shape),
        input_grad.reshape(inputs.shape),
        shares[0],
        shares[1],
        qkv_grad.reshape(row_count, 3, part).transpose(1, 0, 2),
        shares[2],
        shares[3],
        out_grad.T,
        shares[4],
        shares[5],
        shares[6],
        up_grad,
        shares[8],
        down_grad.T,
        shares[7],
    )


def solution(mesh):
    rows = P(BOTH, None, None)
    vector = P(BOTH)
    return jax.shard_map(
        shards,
        mesh=mesh,
        in_specs=(
            rows,
            P("dp"),
            rows,
            vector,
            vector,
            P(None, "dp", "tensor"),
            vector,
            vector,
            P("tensor", "dp"),
            vector,
            vector,
            vector,
            P("dp", "tensor"),
            vector,
            P("tensor", "dp"),
            vector,
        ),
        out_specs=(
            rows,
            rows,
            vector,
            vector,
            P(None, "dp", "tensor"),
            vector,
            vector,
            P("tensor", "dp"),
            vector,
            vector,
            vector,
            P("dp", "tensor"),
            vector,
            P("tensor", "dp"),
            vector,
        ),
        check_vma=False,
    )
```

```python
import functools
import math

import jax
import jax.numpy as jnp
from jax import lax
from jax.experimental import pallas as pl
from jax.experimental.pallas import tpu as pltpu
from jax.sharding import PartitionSpec as P

HEAD_DIM = 64
EPSILON = 1e-06
BOTH = ("dp", "tensor")
MESH = pl.DeviceIdType.MESH
LANES = 128
bf16 = jnp.bfloat16
f32 = jnp.float32
NN = ((1,), (0,))
NT = ((1,), (1,))
TN = ((0,), (0,))


def mm(a, b, dims):
    return lax.dot_general(a, b, (dims, ((), ())), preferred_element_type=f32)


class Place:
    def __init__(self, dp_count):
        self.bits = int(math.log2(dp_count))
        self.dp = lax.axis_index("dp")
        self.tensor = lax.axis_index("tensor")
        self.own = [lax.rem(lax.div(self.dp, 2**k), 2) for k in range(self.bits)]

    def partner(self, stage):
        if stage == "t":
            return {"tensor": 1 - self.tensor}
        return {"dp": self.dp + (1 - 2 * self.own[stage]) * 2**stage}

    def greet(self):
        barrier = pltpu.get_barrier_semaphore()
        stages = list(range(self.bits)) + ["t"]
        for stage in stages:
            pl.semaphore_signal(barrier, inc=1, device_id=self.partner(stage), device_id_type=MESH)
        pl.semaphore_wait(barrier, len(stages))

    def lead(self, done, flipped=None):
        index = []
        for bit in range(self.bits - 1, -1, -1):
            if bit in done:
                index.append(slice(None))
            elif bit == flipped:
                index.append(1 - self.own[bit])
            else:
                index.append(self.own[bit])
        return tuple(index)


def stage_orders(bits):
    far = list(range(bits - 1, 1, -1))
    return (far + [1, "t"], far + ["t", 1], [1] + far + ["t"], ["t"] + far + [1])


class Flow:
    def __init__(self, entry, bits):
        self.matrix, self.first, self.count, which, self.start = entry
        self.order = stage_orders(bits)[which]
        self.stages = len(self.order)

    def remote(self, src, dst, stage, slot):
        return pltpu.make_async_remote_copy(
            src_ref=src,
            dst_ref=dst,
            send_sem=self.send.at[slot],
            recv_sem=self.recv.at[slot],
            device_id=self.place.partner(stage),
            device_id_type=MESH,
        )


class Spread(Flow):
    def __init__(self, entry, bits, base):
        super().__init__(entry, bits)
        self.plane_slot, self.across_slot = [], [base]
        slot, twice = base + 1, 1
        for stage in self.order:
            self.plane_slot.append(slot)
            self.across_slot.append(slot + twice)
            slot += 2 * twice
            if stage == "t":
                twice = 2
        self.end = slot

    def bind(self, place, shard, full, half, send, recv, local):
        self.place, self.shard, self.full, self.half = place, shard, full, half
        self.send, self.recv, self.local = send, recv, local

    def views(self, done, flipped=None):
        place = self.place
        if "t" in done:
            sides = [0, 1]
        elif flipped == "t":
            sides = [1 - place.tensor]
        else:
            sides = [place.tensor]
        lead = place.lead(done, flipped)
        found = []
        for side in sides:
            start = pl.multiple_of(side * self.half + self.first, LANES)
            found.append(self.full.at[lead + (slice(None), pl.ds(start, self.count))])
        return found

    def piece(self):
        return self.shard.at[:, pl.ds(self.first, self.count)]

    def keep(self):
        return pltpu.make_async_copy(self.piece(), self.views(set())[0], self.local)

    def plane(self, step):
        targets = self.views(set(self.order[:step]))
        sources = [self.piece()] if step == 0 else targets
        slot = self.plane_slot[step]
        return [
            self.remote(src, dst, self.order[step], slot + i)
            for i, (src, dst) in enumerate(zip(sources, targets))
        ]

    def across(self, step):
        slot = self.across_slot[step]
        if step == 0:
            return [self.remote(self.piece(), self.views(set())[0], 0, slot)]
        fresh = self.views(set(self.order[: step - 1]), self.order[step - 1])
        return [self.remote(view, view, 0, slot + i) for i, view in enumerate(fresh)]

    def tick(self, step):
        if step == 0:
            self.keep().start()
        else:
            for made in self.plane(step - 1):
                made.wait_recv()
        if step == 1:
            self.keep().wait()
        if step < self.stages:
            for made in self.plane(step):
                made.start()
        for made in self.across(step):
            made.start()

    def finish(self):
        for step in range(self.stages):
            for made in self.plane(step):
                made.wait_send()
        for step in range(self.stages + 1):
            for made in self.across(step):
                made.wait()


class Fold(Flow):
    def __init__(self, entry, bits, base):
        super().__init__(entry, bits)
        self.order = list(reversed(self.order))
        self.base = base
        self.end = base + 2 + self.stages

    def bind(self, place, partial, half, total, landing, result, send, recv, local):
        self.place, self.partial, self.half = place, partial, half
        self.total, self.landing, self.result = total, landing, result
        self.send, self.recv, self.local = send, recv, local

    def loads(self):
        every = set(range(1, self.place.bits))
        made = []
        for side in (0, 1):
            columns = pl.ds(side * self.half + self.first, self.count)
            mine = self.partial.at[self.place.lead(every) + (slice(None), columns)]
            made.append(pltpu.make_async_copy(mine, self.total.at[side], self.local.at[side]))
        return made

    def cores(self):
        every = set(range(1, self.place.bits))
        made = []
        for side in (0, 1):
            columns = pl.ds(side * self.half + self.first, self.count)
            theirs = self.partial.at[self.place.lead(every, 0) + (slice(None), columns)]
            made.append(self.remote(theirs, self.landing[0].at[side], 0, self.base + side))
        return made

    def begin(self):
        for made in self.loads() + self.cores():
            made.start()

    def where(self, done, last=None):
        place = self.place
        index = []
        for name in ["t"] + list(range(place.bits - 1, 0, -1)):
            own = place.tensor if name == "t" else place.own[name]
            if name in done:
                index.append(own)
            elif name == last:
                index.append(1 - own)
            else:
                index.append(None)
        return index

    def stage(self, step):
        index = self.where(set(self.order[:step]), self.order[step])
        view = self.total.at[tuple(slice(None) if e is None else e for e in index)]
        return self.remote(view, self.landing[step + 1], self.order[step], self.base + 2 + step)

    def add(self, landing, done):
        index = self.where(done)
        free = [i for i, entry in enumerate(index) if entry is None]

        def one(j, carry):
            spots, inner = list(index), []
            for position, dim in enumerate(free):
                bit = lax.rem(lax.div(j, 2 ** (len(free) - 1 - position)), 2)
                spots[dim] = bit
                inner.append(bit)
            spots, inner = tuple(spots), tuple(inner)
            value = self.total[spots].astype(f32) + landing[inner].astype(f32)
            self.total[spots] = value.astype(self.total.dtype)
            return carry

        lax.fori_loop(0, 2 ** len(free), one, 0)

    def tick(self, step):
        order = self.order
        if step == 0:
            for made in self.loads():
                made.wait()
            for made in self.cores():
                made.wait_recv()
            self.add(self.landing[0], set())
        else:
            self.stage(step - 1).wait_recv()
            if step < self.stages:
                self.add(self.landing[step], set(order[:step]))
            else:
                spots = tuple(self.where(set(order)))
                value = self.total[spots].astype(f32) + self.landing[step][...].astype(f32)
                self.result[:, self.first : self.first + self.count] = value
        if step < self.stages:
            self.stage(step).start()

    def finish(self):
        for made in self.cores():
            made.wait_send()
        for step in range(self.stages):
            self.stage(step).wait_send()


def fold_scratch(bits, rows, count, dtype):
    lead = (2,) * bits
    shapes = [pltpu.VMEM(lead + (rows, count), dtype)]
    for stage in range(bits + 1):
        shapes.append(pltpu.VMEM(lead[stage:] + (rows, count), dtype))
    return shapes


class Travel:
    def __init__(self, kind, arrays, plan, dp_count):
        self.kind, self.dp_count = kind, dp_count
        self.bits = int(math.log2(dp_count))
        self.flows, base = [], 0
        for entry in plan:
            flow = kind(entry, self.bits, base)
            base = flow.end
            self.flows.append(flow)
        self.count = len(arrays)
        self.ticks = max(flow.start + flow.stages for flow in self.flows) + 1
        any_space = pl.BlockSpec(memory_space=pl.ANY)
        lead = (2,) * self.bits
        self.scratch = [pltpu.SemaphoreType.DMA((base,)), pltpu.SemaphoreType.DMA((base,))]
        if kind is Spread:
            self.operands = list(arrays)
            self.halves = [a.shape[1] for a in arrays]
            self.in_specs = [any_space] * self.count
            self.out_shape = [
                jax.ShapeDtypeStruct(lead + (a.shape[0], 2 * a.shape[1]), a.dtype) for a in arrays
            ]
            self.out_specs = [any_space] * self.count
            self.scratch.append(pltpu.SemaphoreType.DMA((len(plan) + self.count,)))
            self.scratch += [pltpu.VMEM(a.shape, a.dtype) for a in arrays]
        else:
            self.operands = [
                a.reshape(lead + (a.shape[0] // dp_count, a.shape[1])) for a in arrays
            ]
            self.halves = [a.shape[1] // 2 for a in arrays]
            rows = [a.shape[0] // dp_count for a in arrays]
            self.in_specs = [any_space] * self.count
            self.out_shape = [
                jax.ShapeDtypeStruct((r, h), f32) for r, h in zip(rows, self.halves)
            ]
            self.out_specs = [
                pl.BlockSpec((r, h), lambda *g: (0, 0)) for r, h in zip(rows, self.halves)
            ]
            self.scratch.append(pltpu.SemaphoreType.DMA((len(plan), 2)))
            for flow in self.flows:
                a = arrays[flow.matrix]
                self.scratch += fold_scratch(self.bits, rows[flow.matrix], flow.count, a.dtype)

    def bind(self, sources, targets, scratch):
        self.place = Place(self.dp_count)
        send, recv, local = scratch[:3]
        self.local, self.sources, self.held = local, sources, scratch[3:]
        each = self.bits + 2
        for i, flow in enumerate(self.flows):
            m = flow.matrix
            if self.kind is Spread:
                flow.bind(
                    self.place, self.held[m], targets[m], self.halves[m], send, recv, local.at[i]
                )
            else:
                mine = self.held[i * each : (i + 1) * each]
                flow.bind(
                    self.place,
                    sources[m],
                    self.halves[m],
                    mine[0],
                    mine[1:],
                    targets[m],
                    send,
                    recv,
                    local.at[i],
                )

    def begin(self):
        self.place.greet()
        if self.kind is Spread:
            loads = [
                pltpu.make_async_copy(src, dst, self.local.at[len(self.flows) + i])
                for i, (src, dst) in enumerate(zip(self.sources, self.held))
            ]
            for made in loads:
                made.start()
            for made in loads:
                made.wait()
        else:
            for flow in self.flows:
                flow.begin()

    def tick(self, number):
        for flow in self.flows:
            if 0 <= number - flow.start <= flow.stages:
                flow.tick(number - flow.start)

    def finish(self):
        for flow in self.flows:
            flow.finish()

    def results(self, outs):
        if self.kind is Spread:
            return [o.reshape(-1, o.shape[-1]) for o in outs]
        return list(outs)


def carried_kernel(travel, compute, points, steps, ins, outs, *refs):
    n = travel.count
    here = refs[:ins]
    sources = refs[ins : ins + n]
    made = refs[ins + n : ins + n + outs]
    targets = refs[ins + n + outs : ins + 2 * n + outs]
    scratch = refs[ins + 2 * n + outs :]
    travel.bind(sources, targets, scratch[: len(travel.scratch)])
    total = points * steps
    due = {}
    for number in range(travel.ticks):
        due.setdefault(min(number * total // travel.ticks, total - 1), []).append(number)

    def at(point):
        for step in range(steps):
            numbers = due.get(step * points + point, [])
            first = step == 0 and point == 0
            if not numbers and not first:
                continue

            def act(numbers=numbers, first=first):
                if first:
                    travel.begin()
                for number in numbers:
                    travel.tick(number)

            if steps == 1:
                act()
            else:
                pl.when(pl.program_id(0) == step)(act)

    compute(*here, *made, *scratch[len(travel.scratch) :], at)
    if steps == 1:
        travel.finish()
    else:
        pl.when(pl.program_id(0) == steps - 1)(travel.finish)


def carry(travel, collective, name, compute=None, points=1, steps=1, operands=(), in_specs=(),
          out_shape=(), out_specs=(), scratch=(), flops=0, vmem=60):
    if compute is None:

        def compute(at):
            for point in range(points):
                at(point)

    outs = pl.pallas_call(
        functools.partial(
            carried_kernel, travel, compute, points, steps, len(operands), len(out_shape)
        ),
        grid=() if steps == 1 else (steps,),
        out_shape=list(out_shape) + travel.out_shape,
        in_specs=list(in_specs) + travel.in_specs,
        out_specs=list(out_specs) + travel.out_specs,
        scratch_shapes=travel.scratch + list(scratch),
        compiler_params=pltpu.CompilerParams(
            collective_id=collective, has_side_effects=True, vmem_limit_bytes=vmem << 20
        ),
        name=name,
    )(*operands, *travel.operands)
    return list(outs[: len(out_shape)]), travel.results(outs[len(out_shape) :])


def make_plan(sizes, fractions):
    plan, position, tick = [], {}, 0
    for matrix, size in sizes:
        start = position.get(matrix, 0)
        units, total, taken, gone = size // LANES, sum(fractions), 0, 0
        for which, weight in enumerate(fractions):
            taken += weight
            upto = (units * taken * 2 + total) // (2 * total)
            if upto > gone:
                plan.append((matrix, start + gone * LANES, (upto - gone) * LANES, which, tick))
            gone = upto
        position[matrix] = start + size
        tick += 1
    return plan


EVEN = (1, 1, 1, 1)


def chunks(order, halves):
    sizes = []
    for matrix in order:
        half = halves[matrix]
        if half > 1536:
            sizes += [(matrix, half // 2)] * 2
        else:
            sizes.append((matrix, half))
    return sizes


def softmax_rows(scores, valid):
    scores = jnp.where(valid > 0.5, scores, -1000000000.0)
    shifted = jnp.exp(scores - jnp.max(scores, axis=-1, keepdims=True))
    return shifted * (1.0 / jnp.sum(shifted, axis=-1, keepdims=True))


def head_masks():
    lane = lax.broadcasted_iota(jnp.int32, (1, LANES), 1)
    per = LANES // HEAD_DIM
    return [(lane // HEAD_DIM == h).astype(f32).astype(bf16) for h in range(per)], lane


def pick(parts, lane):
    out = parts[0]
    for h in range(1, len(parts)):
        out = jnp.where(lane // HEAD_DIM == h, parts[h], out)
    return out


def attend(first, wq, wk, wv, qb, vb, valid, q_out, k_out, v_out, mix_out, at):
    images, slots = valid.shape[0], valid.shape[2]
    at(0)
    q_out[...] = (mm(first[...], wq[...], NN) + qb[...]).astype(bf16)
    k_out[...] = mm(first[...], wk[...], NN).astype(bf16)
    at(1)
    v_out[...] = (mm(first[...], wv[...], NN) + vb[...]).astype(bf16)
    at(2)
    masks, lane = head_masks()
    point = 3
    for image in range(images):
        rows = slice(image * slots, (image + 1) * slots)
        for pair in range(q_out.shape[1] // LANES):
            columns = slice(pair * LANES, (pair + 1) * LANES)
            query = q_out[rows, columns] * bf16(HEAD_DIM**-0.5)
            key, value = k_out[rows, columns], v_out[rows, columns]
            parts = []
            for mask in masks:
                probs = softmax_rows(mm(query, key * mask, NT), valid[image])
                parts.append(mm(probs.astype(bf16), value, NN))
            mix_out[rows, columns] = pick(parts, lane).astype(bf16)
            at(point)
            point += 1


def attend_back(q, k, v, mixed, grad_attn, grad_attn_t, first_t, out_t, wq, wk, wv, valid,
                out_part, q_part, k_part, v_part, grad_first, qb_grad, vb_grad,
                gm, dq, dk, dv, at):
    images, slots = valid.shape[0], valid.shape[2]
    scale = HEAD_DIM**-0.5
    at(0)
    gm[...] = mm(grad_attn[...], out_t[...], NN).astype(bf16)
    out_part[...] = mm(grad_attn_t[...], mixed[...], NN).astype(bf16)
    at(1)
    masks, lane = head_masks()
    point = 2
    for image in range(images):
        rows = slice(image * slots, (image + 1) * slots)
        for pair in range(q.shape[1] // LANES):
            columns = slice(pair * LANES, (pair + 1) * LANES)
            query = q[rows, columns] * bf16(scale)
            key, value, grad = k[rows, columns], v[rows, columns], gm[rows, columns]
            dqs, dks, dvs = [], [], []
            for mask in masks:
                probs = softmax_rows(mm(query, key * mask, NT), valid[image])
                pulled = mm(grad, value * mask, NT)
                dvs.append(mm(probs.astype(bf16), grad, TN))
                inner = jnp.sum(probs * pulled, axis=-1, keepdims=True)
                grad_scores = (probs * (pulled - inner)).astype(bf16)
                dqs.append(mm(grad_scores, key, NN))
                dks.append(mm(grad_scores, query, TN))
            dq[rows, columns] = (pick(dqs, lane) * scale).astype(bf16)
            dk[rows, columns] = pick(dks, lane).astype(bf16)
            dv[rows, columns] = pick(dvs, lane).astype(bf16)
            at(point)
            point += 1
    qb_grad[...] = jnp.sum(dq[...].astype(f32), axis=0, keepdims=True)
    vb_grad[...] = jnp.sum(dv[...].astype(f32), axis=0, keepdims=True)
    q_part[...] = mm(first_t[...], dq[...], NN).astype(bf16)
    k_part[...] = mm(first_t[...], dk[...], NN).astype(bf16)
    at(point)
    v_part[...] = mm(first_t[...], dv[...], NN).astype(bf16)
    back = mm(dq[...], wq[...], NT) + mm(dk[...], wk[...], NT) + mm(dv[...], wv[...], NT)
    at(point + 1)

    @pl.when(pl.program_id(0) == 0)
    def _():
        grad_first[...] = back

    @pl.when(pl.program_id(0) > 0)
    def _():
        grad_first[...] += back


WIDE = 2 * LANES


def whole(shape):
    return pl.BlockSpec(shape, lambda p: (0,) * len(shape), pipeline_mode=pl.Buffered(1))


def across(rows):
    return pl.BlockSpec((rows, WIDE), lambda p: (0, p))


def attention(travel, collective, first, weights, qbias, vbias, valid):
    tokens, width = first.shape
    shape = jax.ShapeDtypeStruct((tokens, width), bf16)
    images = valid.shape[0]
    return carry(
        travel,
        collective,
        "attention",
        compute=attend,
        points=3 + images * (WIDE // LANES),
        steps=width // WIDE,
        operands=(first, *weights, qbias.reshape(1, -1), vbias.reshape(1, -1), valid),
        in_specs=(
            [whole((tokens, width))]
            + [across(width)] * 3
            + [across(1)] * 2
            + [whole(valid.shape)]
        ),
        out_shape=[shape] * 4,
        out_specs=[across(tokens)] * 4,
    )


def attention_back(travel, collective, q, k, v, mixed, grad_attn, first, out_t, weights, valid):
    tokens, width = first.shape
    images = valid.shape[0]
    part = jax.ShapeDtypeStruct((width, width), bf16)
    vector = jax.ShapeDtypeStruct((1, width), f32)
    return carry(
        travel,
        collective,
        "attention_back",
        compute=attend_back,
        points=4 + images * (WIDE // LANES),
        steps=width // WIDE,
        operands=(q, k, v, mixed, grad_attn, grad_attn.T, first.T, out_t, *weights, valid),
        in_specs=(
            [across(tokens)] * 4
            + [whole((tokens, width)), whole((width, tokens)), whole((width, tokens))]
            + [across(width)] * 4
            + [whole(valid.shape)]
        ),
        out_shape=[part] * 4 + [jax.ShapeDtypeStruct((tokens, width), f32)] + [vector] * 2,
        out_specs=(
            [across(width)] * 4 + [whole((tokens, width))] + [across(1)] * 2
        ),
        scratch=[pltpu.VMEM((tokens, WIDE), bf16)] * 4,
    )


def exact_gelu(values):
    return jax.nn.gelu(values, approximate=False)


def norm_stats(values):
    average = jnp.mean(values, axis=-1, keepdims=True)
    centered = values - average
    variance = jnp.mean(centered * centered, axis=-1, keepdims=True)
    scale = lax.rsqrt(variance + EPSILON)
    return centered * scale, scale


def norm_back(grad, unit, scale, gain):
    z = grad * gain
    mean_z = jnp.mean(z, axis=-1, keepdims=True)
    mean_zx = jnp.mean(z * unit, axis=-1, keepdims=True)
    return scale * (z - mean_z - unit * mean_zx)


def total(values):
    return jnp.sum(values.astype(f32), axis=0)


def shards(
    inputs,
    lengths,
    cotangent,
    first_gain,
    first_shift,
    qkv_weight,
    query_bias,
    value_bias,
    out_weight,
    out_bias,
    second_gain,
    second_shift,
    up_weight,
    up_bias,
    down_weight,
    down_bias,
):
    image_count, slot_count, width = inputs.shape
    tensor_rank = lax.axis_index("tensor")
    tokens = image_count * slot_count
    dp_count = lax.axis_size("dp")
    device_count = dp_count * lax.axis_size("tensor")

    vectors = (
        first_gain,
        first_shift,
        query_bias,
        value_bias,
        out_bias,
        second_gain,
        second_shift,
        down_bias,
        up_bias,
    )
    sizes = [v.shape[0] for v in vectors]
    packed = jnp.concatenate(vectors)
    length = -(-packed.shape[0] // LANES) * LANES
    packed = jnp.pad(packed, (0, length - packed.shape[0]))
    packed = jnp.broadcast_to(packed, (8, length))

    sources = [qkv_weight[0], qkv_weight[1], qkv_weight[2], packed]
    half = qkv_weight.shape[2]
    plan = [(3, 0, length, 2, 0)] + head_plan(half)
    _, (query_w, key_w, value_w, spread) = carry(
        Travel(Spread, sources, plan, dp_count), 1, "spread_first", points=len(plan) + 8
    )
    spread = spread.reshape(dp_count, 8, 2, length)[:, 0].reshape(device_count, length)
    full = []
    start = 0
    for size in sizes:
        full.append(spread[:, start : start + size].reshape(-1).astype(f32))
        start += size
    gain_one, shift_one, qbias, vbias, obias, gain_two, shift_two, dbias, ubias = full

    positions = jnp.arange(slot_count, dtype=jnp.int32)
    own_lengths = lax.dynamic_slice_in_dim(lengths, tensor_rank * image_count, image_count)
    valid = (positions[None, :] < own_lengths[:, None]).astype(f32)
    valid_rows = valid.reshape(tokens, 1)
    masked = inputs.reshape(tokens, width).astype(f32) * valid_rows
    unit_one, scale_one = norm_stats(masked)
    first = (unit_one * gain_one + shift_one).astype(bf16)

    sources = [out_weight.T, up_weight, down_weight.T]
    halves = [s.shape[1] for s in sources]
    plan = make_plan(chunks((0, 1, 2), halves), EVEN)
    valid = valid.reshape(image_count, 1, slot_count)
    qkv_w = (query_w, key_w, value_w)
    (query, key, value, mixed), (out_t, up_w, down_t) = attention(
        Travel(Spread, sources, plan, dp_count), 2, first, qkv_w, qbias, vbias, valid
    )
    middle = masked + mm(mixed, out_t, NT) + obias
    unit_two, scale_two = norm_stats(middle)
    second = (unit_two * gain_two + shift_two).astype(bf16)
    hidden = mm(second, up_w, NN) + ubias
    active = exact_gelu(hidden).astype(bf16)
    output = (middle + mm(active, down_t, NT) + dbias).astype(bf16)

    grad_low = cotangent.reshape(tokens, width)
    grad_out = grad_low.astype(f32)
    down_part = mm(grad_low, active, TN).astype(bf16)
    grad_active = mm(grad_low, down_t, NN)
    grad_hidden = jax.vjp(exact_gelu, hidden)[1](grad_active)[0].astype(bf16)
    up_part = mm(second, grad_hidden, TN).astype(bf16)
    grad_second = mm(grad_hidden, up_w, NT)
    grad_middle = grad_out + norm_back(grad_second, unit_two, scale_two, gain_two)
    grad_attn = grad_middle.astype(bf16)

    sources = [down_part, up_part]
    halves = [s.shape[1] // 2 for s in sources]
    plan = make_plan(chunks((0, 1), halves), EVEN)
    (out_part, q_part, k_part, v_part, grad_first, qb_grad, vb_grad), (down_grad, up_grad) = (
        attention_back(
            Travel(Fold, sources, plan, dp_count),
            3,
            query,
            key,
            value,
            mixed,
            grad_attn,
            first,
            out_t,
            qkv_w,
            valid,
        )
    )
    grad_in = norm_back(grad_first, unit_one, scale_one, gain_one)
    input_grad = (grad_middle + grad_in) * valid_rows

    vector_grads = (
        total(grad_first * unit_one),
        total(grad_first),
        qb_grad,
        vb_grad,
        total(grad_attn),
        total(grad_second * unit_two),
        total(grad_second),
        total(grad_low),
        total(grad_hidden),
    )
    stacked = jnp.concatenate([v.reshape(device_count, -1) for v in vector_grads], axis=1)
    stacked = jnp.pad(stacked, ((0, 0), (0, length - stacked.shape[1])))
    stacked = stacked.reshape(-1, 1, 2 * length)
    stacked = jnp.pad(stacked, ((0, 0), (0, 7), (0, 0))).reshape(-1, 2 * length)
    sources = [q_part, k_part, v_part, stacked, out_part]
    plan = make_plan([(4, half)], EVEN) + head_plan(half, 1) + [(3, 0, length, 2, 2)]
    _, (q_grad, k_grad, v_grad, own, out_grad) = carry(
        Travel(Fold, sources, plan, dp_count), 4, "fold_last", points=10
    )
    own = own[0]
    shares = []
    start = 0
    for size in sizes:
        shares.append(own[start : start + size])
        start += size

    return (
        output.reshape(inputs.shape),
        input_grad.reshape(inputs.shape),
        shares[0],
        shares[1],
        jnp.stack([q_grad, k_grad, v_grad]),
        shares[2],
        shares[3],
        out_grad.T,
        shares[4],
        shares[5],
        shares[6],
        up_grad,
        shares[8],
        down_grad.T,
        shares[7],
    )


def head_plan(half, start=0):
    plan = []
    for matrix, shares in ((0, (1, 1, 0, 0)), (1, (0, 0, 1, 1)), (2, EVEN)):
        for entry in make_plan([(matrix, half)], shares):
            plan.append(entry[:4] + (start + matrix // 2,))
    return plan


def solution(mesh):
    rows = P(BOTH, None, None)
    vector = P(BOTH)
    return jax.shard_map(
        shards,
        mesh=mesh,
        in_specs=(
            rows,
            P("dp"),
            rows,
            vector,
            vector,
            P(None, "dp", "tensor"),
            vector,
            vector,
            P("tensor", "dp"),
            vector,
            vector,
            vector,
            P("dp", "tensor"),
            vector,
            P("tensor", "dp"),
            vector,
        ),
        out_specs=(
            rows,
            rows,
            vector,
            vector,
            P(None, "dp", "tensor"),
            vector,
            vector,
            P("tensor", "dp"),
            vector,
            vector,
            vector,
            P("dp", "tensor"),
            vector,
            P("tensor", "dp"),
            vector,
        ),
        check_vma=False,
    )
```
